32 devices in a mesh: ev: 2 (over core), own: 16 (over z, y, x).
Axes of the slice: x: 2, y: 2, z: 4, core: 2. Of those that a mesh axis runs over, the one named last changes fastest.
Arguments:
- ground_up: bfloat16 [8192, 4096], P('own', 'ev'), parts along dimension 1, may hold values from 0.049804688 to 2
- item_site: int32 [8192], P('own'), may hold values from 0 to 127
- item_profile: int32 [8192], P('own'), may hold values from 0 to 127
- site_owner: int32 [2048, 1], P('own'), may hold values from 0 to 15; in each aligned block of 128 rows (0 to 127, 128 to 255, ...) at most 16 rows name the same one
- site_slot: int32 [2048], P('own'), may hold values from 0 to 63
- site_profile: int32 [2048], P('own'), may hold values from 0 to 127
- policy_owner: int32 [1024, 1], P('own'), may hold values from 0 to 15; in each aligned block of 64 rows (0 to 63, 64 to 127, ...) at most 12 rows name the same one
- policy_slot: int32 [1024], P('own'), may hold values from 0 to 1
- policy_profile: int32 [1024], P('own'), may hold values from 0 to 127
- program_profile: int32 [32], P('own'), may hold values from 0 to 127
- term_table: float32 [4, 3, 128], replicated, may hold values from 0 to 90, as said below
Outputs:
- policy_loss: bfloat16 [1024, 4096], P('own', 'ev'), parts along dimension 1
- program_loss: float32 [32, 4096], P('own', 'ev'), parts along dimension 1
The draws below stay inside these ranges and needn't reach their ends.
There are 2 independent parts, one for each index of `ev`. The reference program is written for one: setup_inputs(seed, part) draws one part's arguments, and reference() takes and returns one part's arrays. A program takes and returns all parts, laid end to end along the dimension named above; an argument that names none is the same for every part. Nothing has to cross between parts.
Inputs may be any that keep to these rules, and one draw needn't show every extreme that they name: `site_owner`: among the 128 sites of one owner, no owner of policies appears more than 16 times; some owner appears exactly 16 times in some owner's sites. `policy_owner`: among the 64 policies of one owner, no owner of programs appears more than 12 times; some owner appears exactly 12 times in some owner's policies. `term_table`: deductibles are 0 or more, limits positive, shares between 0.5 and 1.
All inputs are finite; a program needn't handle non-finite values.
Results may differ from the reference program's by a relative error of at most 0.0051.
Values may be sent and summed in bfloat16 or wider, within the bound.
A program may use at most 64 MiB of HBM per device.

```python
import math
import jax
import jax.numpy as jnp
import numpy as np
from jax import lax

ROWS = 2048
ITEM_DEV = 512
SITE_DEV = 128
POL_DEV = 64
PROG_DEV = 2
PROFILES = 128
ITEMS = 8192
SITES = 2048
POLICIES = 1024
PROGRAMS = 32
CAP = 16
PROG_CAP = 12
N_OWN = 16


def draw_term_table(key, part):
    deduct_top = jnp.array([0.3, 1.0, 1.0, 20.0], jnp.float32)
    ceiling_low = jnp.array([0.5, 1.0, 2.0, 30.0], jnp.float32)
    ceiling_top = jnp.array([1.5, 4.0, 6.0, 90.0], jnp.float32)
    uniforms = jax.random.uniform(key, (4, 3, PROFILES), jnp.float32)
    deduct = uniforms[:, 0] * deduct_top[:, None]
    ceiling = ceiling_low[:, None] + uniforms[:, 1] * (ceiling_top - ceiling_low)[:, None]
    portion = 0.5 + 0.5 * uniforms[:, 2]
    return jnp.stack([deduct, ceiling, portion], axis=1)


def with_ends(values, key, least, largest):
    longest = values.shape.index(max(values.shape))
    spots = []
    for shift in (0, 1):
        where = [jax.random.randint(jax.random.fold_in(key, axis), (), 0, length) for axis, length in enumerate(values.shape)]
        where[longest] = (where[longest] + shift) % values.shape[longest]
        spots.append(tuple(where))
    return values.at[spots[0]].set(least).at[spots[1]].set(largest)


def block_scale(rng, shape, pieces, low, top_value):
    gain, own = 1.0, jax.random.fold_in(rng, 6)
    for dim, parts in pieces:
        steps = jnp.exp(jax.random.uniform(jax.random.fold_in(own, dim), (parts,), jnp.float32, low / len(pieces), top_value / len(pieces)))
        gain = gain * jnp.repeat(steps, shape[dim] // parts).reshape([-1 if axis == dim else 1 for axis in range(len(shape))])
    return gain


def rank_table(amount, lean):
    loads = [(1 << 20) // math.isqrt(standing ** lean) + 1 for standing in range(1, amount + 1)]
    width = 1 + sum(loads) // (1 << 30)
    return np.cumsum(np.array([max(1, weight // width) for weight in loads]))


def ranked(key, dims, number_of, skew):
    listing = rank_table(number_of, skew)
    ticket = jax.random.randint(jax.random.fold_in(key, 1), dims, 0, int(listing[number_of - 1]))
    rank = jnp.searchsorted(jnp.asarray(listing, jnp.int32), ticket, side="right")
    return jax.random.permutation(jax.random.fold_in(key, 2), number_of)[rank].astype(jnp.int32)


def shared_out(rng, own, number, rows, count, top, reach, skew):
    sequence = jax.random.permutation(rng, count)
    heavy_load, common = load_shares(count, rows * top, reach, skew, True), load_shares(count, rows * top, reach, skew, False)
    places = jnp.arange(count)

    def named(tallies, rotation):
        used = int((tallies > 0).sum())
        fixed = max(1, used // 4)
        shifted = fixed + (places - fixed + rotation * (used - fixed)) % max(1, count - fixed)
        return jnp.zeros((count,), jnp.int32).at[sequence[jnp.where(places < fixed, places, shifted)]].set(jnp.asarray(tallies, jnp.int32))

    tallies = jnp.where(number % 4 == 0, named(heavy_load, number // 4), named(common, number - number // 4 - 1))
    mixed = jax.random.permutation(jax.random.fold_in(own, 3), count)
    donor, taker = mixed[0:count // 2 * 2:2], mixed[1:count // 2 * 2:2]
    margin = jnp.minimum(tallies[donor] - 1, reach - tallies[taker]) // 2
    margin = jnp.where((donor == sequence[0]) | (taker == sequence[0]) | (tallies[taker] == 0), 0, jnp.maximum(margin, 0))
    shifted = jax.random.randint(jax.random.fold_in(own, 4), (count // 2,), 0, 1 << 20) % (margin + 1)
    tallies = tallies.at[donor].add(-shifted).at[taker].add(shifted)
    items = jnp.searchsorted(jnp.cumsum(tallies), jnp.arange(rows * top), side="right").astype(jnp.int32)
    listing = items.reshape(top, rows).T
    listing = listing[jax.random.permutation(jax.random.fold_in(own, 1), rows)]
    rotation = jax.random.randint(jax.random.fold_in(own, 2), (rows, 1), 0, top)
    return jnp.take_along_axis(listing, (jnp.arange(top)[None, :] + rotation) % top, axis=1)


def load_shares(number_of, total, reach, skew, full):
    weights = [(1 << 20) // math.isqrt(standing ** skew) + 1 for standing in range(1, number_of + 1)]
    largest = reach if full else min(reach, max(-(-total // number_of), total * weights[0] // sum(weights)))
    least = 1 if total - largest >= number_of - 1 else 0
    given, spare = [largest] + [least] * (number_of - 1), total - largest - least * (number_of - 1)
    while spare > 0:
        movable = [i for i in range(1, number_of) if given[i] < largest] or [i for i in range(1, number_of) if given[i] < reach]
        pool, remaining = sum([weights[i] for i in movable]), spare
        for i in movable:
            extra = min(reach - given[i], max(1, remaining * weights[i] // pool), spare)
            given[i] = given[i] + extra
            spare = spare - extra
    return np.array(given)


def setup_inputs(seed: int = 0, part: int = 0) -> dict:
    splits = jax.random.split(jax.random.key(seed), 12)
    own_keys = jax.random.split(jax.random.fold_in(splits[11], part), 12)
    ground_up = jnp.clip(jnp.exp(math.log(2.0) - 3.6927934 * jax.random.uniform(own_keys[0], (ITEMS, ROWS), jnp.float32) ** block_scale(own_keys[0], (ITEMS, ROWS), ((0, 16),), -0.2, 0.2)), 0.049804688, 2.0).astype(jnp.bfloat16)
    item_site = with_ends(ranked(splits[1], (ITEMS,), SITE_DEV, 1), jax.random.fold_in(splits[1], 3), 0, SITE_DEV - 1).astype(jnp.int32)
    item_profile = with_ends(jax.random.randint(splits[2], (ITEMS,), 0, PROFILES), jax.random.fold_in(splits[2], 1), 0, PROFILES - 1).astype(jnp.int32)
    site_owner_keys = jax.random.split(jax.random.fold_in(splits[3], 1), SITES // SITE_DEV)
    site_owner_turns = jax.random.permutation(jax.random.fold_in(splits[3], 3), SITES // SITE_DEV)
    site_owner = jax.vmap(lambda own, number: shared_out(jax.random.fold_in(splits[3], 2), own, number, SITE_DEV, N_OWN, 1, CAP, 2))(site_owner_keys, site_owner_turns).reshape((SITES, 1))
    site_slot = with_ends(jax.random.randint(splits[4], (SITES,), 0, POL_DEV), jax.random.fold_in(splits[4], 1), 0, POL_DEV - 1).astype(jnp.int32)
    site_profile = with_ends(jax.random.randint(splits[5], (SITES,), 0, PROFILES), jax.random.fold_in(splits[5], 1), 0, PROFILES - 1).astype(jnp.int32)
    policy_owner_keys = jax.random.split(jax.random.fold_in(splits[6], 1), POLICIES // POL_DEV)
    policy_owner_turns = jax.random.permutation(jax.random.fold_in(splits[6], 3), POLICIES // POL_DEV)
    policy_owner = jax.vmap(lambda own, number: shared_out(jax.random.fold_in(splits[6], 2), own, number, POL_DEV, N_OWN, 1, PROG_CAP, 2))(policy_owner_keys, policy_owner_turns).reshape((POLICIES, 1))
    policy_slot = with_ends(jax.random.randint(splits[7], (POLICIES,), 0, PROG_DEV), jax.random.fold_in(splits[7], 1), 0, PROG_DEV - 1).astype(jnp.int32)
    policy_profile = with_ends(jax.random.randint(splits[8], (POLICIES,), 0, PROFILES), jax.random.fold_in(splits[8], 1), 0, PROFILES - 1).astype(jnp.int32)
    program_profile = with_ends(jax.random.randint(splits[9], (PROGRAMS,), 0, PROFILES), jax.random.fold_in(splits[9], 1), 0, PROFILES - 1).astype(jnp.int32)
    term_table = draw_term_table(jax.random.fold_in(splits[11], 71), part)
    return dict(ground_up=ground_up, item_site=item_site, item_profile=item_profile, site_owner=site_owner, site_slot=site_slot, site_profile=site_profile, policy_owner=policy_owner, policy_slot=policy_slot, policy_profile=policy_profile, program_profile=program_profile, term_table=term_table)


def apply_terms(gross_loss, terms_table, tier_index, profile):
    deduct = terms_table[tier_index, 0][profile][:, None]
    ceiling = terms_table[tier_index, 1][profile][:, None]
    portion = terms_table[tier_index, 2][profile][:, None]
    return portion * jnp.minimum(jnp.maximum(gross_loss - deduct, 0.0), ceiling)


def reference(ground_up, item_site, item_profile, site_owner, site_slot, site_profile, policy_owner, policy_slot, policy_profile, program_profile, term_table):
    def site_block(inputs):
        losses, local_sites, profiles = inputs
        covered = apply_terms(losses.astype(jnp.float32), term_table, 0, profiles).astype(jnp.bfloat16)
        return jax.ops.segment_sum(covered.astype(jnp.float32), local_sites, num_segments=SITE_DEV)

    site_gross = lax.map(site_block, (ground_up.reshape(N_OWN, ITEM_DEV, ROWS), item_site.reshape(N_OWN, ITEM_DEV), item_profile.reshape(N_OWN, ITEM_DEV)))
    site_gross = site_gross.reshape(SITES, ROWS)
    site_net = apply_terms(site_gross, term_table, 1, site_profile).astype(jnp.bfloat16)
    policy_ids = (site_owner[:, 0] * POL_DEV + site_slot).astype(jnp.int32)
    policy_gross = jax.ops.segment_sum(site_net.astype(jnp.float32), policy_ids, num_segments=POLICIES)
    policy_loss = apply_terms(policy_gross, term_table, 2, policy_profile).astype(jnp.bfloat16)
    program_ids = (policy_owner[:, 0] * PROG_DEV + policy_slot).astype(jnp.int32)
    program_gross = jax.ops.segment_sum(policy_loss.astype(jnp.float32), program_ids, num_segments=PROGRAMS)
    program_loss = apply_terms(program_gross, term_table, 3, program_profile)
    return (policy_loss, program_loss)
```

```python
import functools

import jax
import jax.numpy as jnp
from jax import lax
from jax.experimental import pallas as pl
from jax.experimental.pallas import tpu as pltpu
from jax.sharding import PartitionSpec as P

LANES = 128
META = 8
f32 = jnp.float32
bf16 = jnp.bfloat16


def terms(x, deduct, ceiling, portion):
    return portion * jnp.minimum(jnp.maximum(x - deduct, 0.0), ceiling)


def kernel(
    n,
    pol,
    prog,
    ground,
    ints,
    table,
    policy_out,
    program_out,
    chunks,
    square,
    item_terms,
    site_terms,
    policy_terms,
    program_terms,
    grouping,
    meta,
    send,
    recv,
    acc,
    losses,
    program_send,
    load_sem,
    meta_ss,
    meta_rs,
    site_ss,
    site_rs,
    pol_ss,
    pol_rs,
    prog_ss,
    prog_rs,
):
    me = lax.axis_index("own")
    groups = n // 2
    mine = me // 2
    half = groups // 2
    items = ground.shape[0]
    blocks = items // LANES
    sites = send.shape[1]
    width = send.shape[2]
    wide = 2 * width

    barrier = pltpu.get_barrier_semaphore()

    def greet(k, c):
        pl.semaphore_signal(barrier, inc=1, device_id={"own": lax.rem(me + k, n)})
        return c

    lax.fori_loop(1, n, greet, 0)

    def load(i):
        g = lax.rem(mine + half + i, groups)
        return pltpu.make_async_copy(
            ground.at[:, pl.ds(pl.multiple_of(g * wide, wide), wide)],
            chunks.at[i],
            load_sem.at[i],
        )

    def start_load(i, c):
        load(i).start()
        return c

    lax.fori_loop(0, groups, start_load, 0)

    square[...] = jnp.zeros_like(square)
    for level in range(4):
        square[3 * level : 3 * level + 3, :] = table[level]
    columns = square[...].T
    rows_iota = lax.broadcasted_iota(jnp.int32, (LANES, LANES), 0)

    def look(profile_row, level):
        pick = rows_iota == profile_row
        return [
            jnp.sum(
                jnp.where(pick, columns[:, 3 * level + t : 3 * level + t + 1], 0.0),
                axis=0,
                keepdims=True,
            )
            for t in range(3)
        ]

    base = 2 * blocks
    own_meta = [ints[base : base + 1, :].astype(f32)]
    own_meta += look(ints[base + 2 : base + 3, :], 2)
    own_meta += [ints[base + 3 : base + 4, :].astype(f32)]
    own_meta += look(ints[base + 4 : base + 5, :], 3)
    meta[me] = jnp.concatenate(own_meta, axis=0)

    for b in range(blocks):
        grouping[:, b * LANES : (b + 1) * LANES] = (rows_iota == ints[b : b + 1, :]).astype(bf16)
        for t, row in enumerate(look(ints[blocks + b : blocks + b + 1, :], 0)):
            square[3 * b + t : 3 * b + t + 1, :] = row
    for t, row in enumerate(look(ints[base + 1 : base + 2, :], 1)):
        square[3 * blocks + t : 3 * blocks + t + 1, :] = row
    flipped = square[...].T
    for t in range(3):
        for b in range(blocks):
            item_terms[t, b * LANES : (b + 1) * LANES, :] = jnp.broadcast_to(
                flipped[:, 3 * b + t : 3 * b + t + 1], (LANES, LANES)
            )
        site_terms[t] = jnp.broadcast_to(
            flipped[:, 3 * blocks + t : 3 * blocks + t + 1], (LANES, LANES)
        )

    pl.semaphore_wait(barrier, n - 1)

    def meta_copy(d, s):
        return pltpu.make_async_remote_copy(
            meta.at[s], meta.at[s], meta_ss.at[d], meta_rs.at[s], device_id={"own": d}
        )

    def site_copy(d, s):
        return pltpu.make_async_remote_copy(
            send.at[d], recv.at[s], site_ss.at[d], site_rs.at[s], device_id={"own": d}
        )

    def policy_copy(d, s):
        return pltpu.make_async_remote_copy(
            losses.at[pl.ds(pl.multiple_of(d * pol, pol), pol), :],
            policy_out.at[:, pl.ds(pl.multiple_of(s * width, width), width)],
            pol_ss.at[d],
            pol_rs.at[s],
            device_id={"own": d},
        )

    def program_copy(d, s):
        return pltpu.make_async_remote_copy(
            program_send.at[d],
            program_out.at[:, pl.ds(pl.multiple_of(s * width, width), width)],
            prog_ss.at[d],
            prog_rs.at[s],
            device_id={"own": d},
        )

    def others(fn):
        def step(k, c):
            fn(lax.rem(me + k, n))
            return c

        lax.fori_loop(1, n, step, 0)

    others(lambda d: meta_copy(d, me).start())

    def sites_step(i, c):
        load(i).wait()
        g = lax.rem(mine + half + i, groups)
        spread = [jnp.concatenate([item_terms[t]] * (wide // LANES), axis=1) for t in range(3)]
        covered = terms(chunks[i].astype(f32), *spread).astype(bf16)
        gross = jnp.dot(grouping[...], covered, preferred_element_type=f32)
        site_spread = [jnp.concatenate([site_terms[t]] * (wide // LANES), axis=1) for t in range(3)]
        net = terms(gross, *site_spread).astype(bf16)
        for j in range(2):
            d = 2 * g + j
            piece = net[:, j * width : (j + 1) * width]

            @pl.when(d == me)
            def _():
                recv[me] = piece

            @pl.when(d != me)
            def _():
                send[d] = piece
                site_copy(d, me).start()

        return c

    lax.fori_loop(0, groups, sites_step, 0)

    others(lambda s: meta_copy(me, s).wait_recv())

    meta_flat = meta[...].reshape(n * META, LANES)
    turned = meta_flat.T
    for o in range(n):
        for t in range(3):
            lane = o * META + 1 + t
            policy_terms[t, o * pol : (o + 1) * pol, :] = jnp.broadcast_to(
                turned[0:pol, lane : lane + 1], (pol, LANES)
            )
            lane = o * META + 5 + t
            program_terms[o, t] = jnp.broadcast_to(turned[0:prog, lane : lane + 1], (prog, LANES))

    policy_iota = lax.broadcasted_iota(jnp.int32, (n * pol, sites), 0).astype(f32)
    order = [0]
    for k in range(1, half + 1):
        order += [k] if k == groups - k else [k, groups - k]
    acc[...] = jnp.zeros_like(acc)

    for k in order:
        g = lax.rem(mine + k, groups)
        for j in range(2):
            s = 2 * g + j

            @pl.when(s != me)
            def _():
                site_copy(me, s).wait_recv()

        pick = jnp.concatenate(
            [(policy_iota == meta[2 * g + j][0:1, :]).astype(bf16) for j in range(2)], axis=1
        )
        values = recv[pl.ds(2 * g, 2)].reshape(2 * sites, width)
        acc[...] += jnp.dot(pick, values, preferred_element_type=f32)

    def policy_step(i, c):
        d = lax.rem(me + n // 2 + i, n)
        at = pl.ds(pl.multiple_of(d * pol, pol), pol)
        spread = [
            jnp.concatenate([policy_terms[t, at, :]] * (width // LANES), axis=1) for t in range(3)
        ]
        losses[at, :] = terms(acc[at, :], *spread).astype(bf16)

        @pl.when(d != me)
        def _():
            policy_copy(d, me).start()

        return c

    lax.fori_loop(0, n, policy_step, 0)
    own_policy = pltpu.make_async_copy(
        losses.at[pl.ds(pl.multiple_of(me * pol, pol), pol), :],
        policy_out.at[:, pl.ds(pl.multiple_of(me * width, width), width)],
        pol_rs.at[me],
    )
    own_policy.start()

    program_iota = lax.broadcasted_iota(jnp.int32, (n * prog, pol), 0).astype(f32)
    marks = [
        (program_iota == meta_flat[o * META + 4 : o * META + 5, 0:pol]).astype(bf16)
        for o in range(n)
    ]
    program_gross = jnp.dot(jnp.concatenate(marks, axis=1), losses[...], preferred_element_type=f32)
    for o in range(n):
        spread = [
            jnp.concatenate([program_terms[o, t]] * (width // LANES), axis=1) for t in range(3)
        ]
        program_send[o] = terms(program_gross[o * prog : (o + 1) * prog, :], *spread)
    others(lambda d: program_copy(d, me).start())
    own_program = pltpu.make_async_copy(
        program_send.at[me],
        program_out.at[:, pl.ds(pl.multiple_of(me * width, width), width)],
        prog_rs.at[me],
    )
    own_program.start()

    def finish(d):
        meta_copy(d, me).wait_send()
        site_copy(d, me).wait_send()
        policy_copy(d, me).wait_send()
        program_copy(d, me).wait_send()
        policy_copy(me, d).wait_recv()
        program_copy(me, d).wait_recv()

    others(finish)
    own_policy.wait()
    own_program.wait()


def exchange(
    ground_up,
    item_site,
    item_profile,
    site_owner,
    site_slot,
    site_profile,
    policy_owner,
    policy_slot,
    policy_profile,
    program_profile,
    term_table,
):
    n = lax.axis_size("own")
    items, cols = ground_up.shape
    sites = site_profile.shape[0]
    pol = policy_profile.shape[0]
    prog = program_profile.shape[0]
    width = cols // n
    blocks = items // LANES

    def row(v):
        return jnp.pad(v, (0, LANES - v.shape[0])).reshape(1, LANES)

    ints = jnp.concatenate(
        [
            item_site.reshape(blocks, LANES),
            item_profile.reshape(blocks, LANES),
            row(site_owner[:, 0] * pol + site_slot),
            row(site_profile),
            row(policy_profile),
            row(policy_owner[:, 0] * prog + policy_slot),
            row(program_profile),
        ],
        axis=0,
    )
    vmem = pl.BlockSpec(memory_space=pltpu.VMEM)
    anyspec = pl.BlockSpec(memory_space=pl.ANY)
    dma = pltpu.SemaphoreType.DMA
    return pl.pallas_call(
        functools.partial(kernel, n, pol, prog),
        out_shape=(
            jax.ShapeDtypeStruct((pol, cols), bf16),
            jax.ShapeDtypeStruct((prog, cols), f32),
        ),
        in_specs=[anyspec, vmem, vmem],
        out_specs=(anyspec, anyspec),
        scratch_shapes=[
            pltpu.VMEM((n // 2, items, 2 * width), bf16),
            pltpu.VMEM((LANES, LANES), f32),
            pltpu.VMEM((3, items, LANES), f32),
            pltpu.VMEM((3, sites, LANES), f32),
            pltpu.VMEM((3, n * pol, LANES), f32),
            pltpu.VMEM((n, 3, prog, LANES), f32),
            pltpu.VMEM((sites, items), bf16),
            pltpu.VMEM((n, META, LANES), f32),
            pltpu.VMEM((n, sites, width), bf16),
            pltpu.VMEM((n, sites, width), bf16),
            pltpu.VMEM((n * pol, width), f32),
            pltpu.VMEM((n * pol, width), bf16),
            pltpu.VMEM((n, prog, width), f32),
            dma((n // 2,)),
        ]
        + [dma((n,))] * 8,
        compiler_params=pltpu.CompilerParams(collective_id=0, has_side_effects=True),
        name="loss_terms",
    )(ground_up, ints, term_table)


def apply_terms(gross_loss, terms_table, tier_index, profile):
    profile_iota = jnp.arange(terms_table.shape[2], dtype=jnp.int32)
    picker = profile[:, None] == profile_iota[None, :]
    deduct = jnp.sum(jnp.where(picker, terms_table[tier_index, 0][None, :], 0.0), axis=1)[:, None]
    ceiling = jnp.sum(jnp.where(picker, terms_table[tier_index, 1][None, :], 0.0), axis=1)[:, None]
    portion = jnp.sum(jnp.where(picker, terms_table[tier_index, 2][None, :], 0.0), axis=1)[:, None]
    return portion * jnp.minimum(jnp.maximum(gross_loss - deduct, 0.0), ceiling)


def pack_rows(values, target_dev, inner_slot, owners, capacity):
    member = (target_dev[:, None] == jnp.arange(owners, dtype=jnp.int32)[None, :]).astype(jnp.int32)
    before = jnp.cumsum(member, axis=0) - member
    position = jnp.sum(before * member, axis=1)
    target = target_dev * capacity + position
    placer = jnp.arange(owners * capacity, dtype=jnp.int32)[:, None] == target[None, :]
    packed = jnp.dot(
        placer.astype(jnp.bfloat16), values, preferred_element_type=jnp.float32
    ).astype(jnp.bfloat16)
    labels = jnp.sum(jnp.where(placer, (inner_slot + 1)[None, :], 0), axis=1) - 1
    return (
        packed.reshape(owners, capacity, values.shape[1]),
        labels.astype(jnp.bfloat16).reshape(owners, capacity),
    )


def sum_rows(received, labels, slot_count):
    flattened = received.reshape(-1, received.shape[2])
    slot_marks = labels.reshape(-1).astype(jnp.int32)
    picker = (jnp.arange(slot_count, dtype=jnp.int32)[:, None] == slot_marks[None, :]).astype(
        jnp.bfloat16
    )
    return jnp.dot(picker, flattened, preferred_element_type=jnp.float32)


def shards(
    ground_up,
    item_site,
    item_profile,
    site_owner,
    site_slot,
    site_profile,
    policy_owner,
    policy_slot,
    policy_profile,
    program_profile,
    term_table,
):
    owners = lax.axis_size("own")
    covered = apply_terms(ground_up.astype(jnp.float32), term_table, 0, item_profile).astype(
        jnp.bfloat16
    )
    site_total = site_profile.shape[0]
    grouping = (jnp.arange(site_total, dtype=jnp.int32)[:, None] == item_site[None, :]).astype(
        jnp.bfloat16
    )
    site_gross = jnp.dot(grouping, covered, preferred_element_type=jnp.float32)
    site_net = apply_terms(site_gross, term_table, 1, site_profile).astype(jnp.bfloat16)
    capacity = 2 * site_total // owners
    packed, labels = pack_rows(site_net, site_owner[:, 0], site_slot, owners, capacity)
    arrived, arrived_labels = (
        lax.all_to_all(packed, "own", split_axis=0, concat_axis=0, tiled=True),
        lax.all_to_all(labels, "own", split_axis=0, concat_axis=0, tiled=True),
    )
    policy_total = policy_profile.shape[0]
    policy_gross = sum_rows(arrived, arrived_labels, policy_total)
    policy_loss = apply_terms(policy_gross, term_table, 2, policy_profile).astype(jnp.bfloat16)
    program_total = program_profile.shape[0]
    program_capacity = 3 * policy_total // owners
    sent_rows, sent_labels = pack_rows(
        policy_loss, policy_owner[:, 0], policy_slot, owners, program_capacity
    )
    got_rows, got_labels = (
        lax.all_to_all(sent_rows, "own", split_axis=0, concat_axis=0, tiled=True),
        lax.all_to_all(sent_labels, "own", split_axis=0, concat_axis=0, tiled=True),
    )
    program_gross = sum_rows(got_rows, got_labels, program_total)
    program_loss = apply_terms(program_gross, term_table, 3, program_profile)
    return (policy_loss, program_loss)


def solution(mesh):
    placed = (
        P("own", "ev"),
        P("own"),
        P("own"),
        P("own", None),
        P("own"),
        P("own"),
        P("own", None),
        P("own"),
        P("own"),
        P("own"),
        P(),
    )

    def body(ground_up, item_site, item_profile, *rest):
        n = lax.axis_size("own")
        items, cols = ground_up.shape
        sites, pol = rest[2].shape[0], rest[5].shape[0]
        prog = rest[6].shape[0]
        fits = cols % (n * LANES) == 0 and items % LANES == 0 and sites == LANES
        fits = fits and pol <= LANES and pol % 16 == 0 and prog <= 8
        fits = fits and n % 4 == 0 and n * META <= LANES and 3 * items <= LANES * (LANES - 3)
        return (exchange if fits else shards)(ground_up, item_site, item_profile, *rest)

    return jax.shard_map(
        body,
        mesh=mesh,
        in_specs=placed,
        out_specs=(P("own", "ev"), P("own", "ev")),
        check_vma=False,
    )
```

```python
import functools

import jax
import jax.numpy as jnp
from jax import lax
from jax.experimental import pallas as pl
from jax.experimental.pallas import tpu as pltpu
from jax.sharding import PartitionSpec as P

LANES = 128
META = 8
SMALL = 10
f32 = jnp.float32
bf16 = jnp.bfloat16


def terms(x, deduct, ceiling, portion):
    return portion * jnp.minimum(jnp.maximum(x - deduct, 0.0), ceiling)


def kernel(
    n,
    pol,
    prog,
    ground,
    *refs,
):
    small_in, refs = refs[:SMALL], refs[SMALL:]
    policy_out, program_out = refs[:2]
    small, refs = refs[2 : 2 + SMALL], refs[2 + SMALL :]
    (
        chunks,
        ids,
        square,
        item_terms,
        site_terms,
        policy_terms,
        program_terms,
        grouping,
        meta,
        send,
        recv,
        acc,
        losses,
        program_send,
        small_sem,
        load_sem,
        meta_ss,
        meta_rs,
        site_ss,
        site_rs,
        pol_ss,
        pol_rs,
        prog_ss,
        prog_rs,
    ) = refs
    me = lax.axis_index("own")
    groups = n // 2
    mine = me // 2
    half = groups // 2
    items = ground.shape[0]
    blocks = items // LANES
    sites = send.shape[1]
    width = send.shape[2]
    wide = 2 * width

    barrier = pltpu.get_barrier_semaphore()

    def greet(k, c):
        pl.semaphore_signal(barrier, inc=1, device_id={"own": lax.rem(me + k, n)})
        return c

    lax.fori_loop(1, n, greet, 0)

    def fetch(i):
        return pltpu.make_async_copy(small_in[i], small[i], small_sem.at[i])

    for i in range(SMALL):
        fetch(i).start()

    def load(i):
        g = lax.rem(mine + half + i, groups)
        return pltpu.make_async_copy(
            ground.at[:, pl.ds(pl.multiple_of(g * wide, wide), wide)],
            chunks.at[i],
            load_sem.at[i],
        )

    def start_load(i, c):
        load(i).start()
        return c

    lax.fori_loop(0, groups, start_load, 0)
    (
        item_site,
        item_profile,
        site_owner,
        site_slot,
        site_profile,
        policy_owner,
        policy_slot,
        policy_profile,
        program_profile,
        table,
    ) = small
    for i in range(SMALL):
        fetch(i).wait()

    square[...] = jnp.zeros_like(square)
    for t in range(3):
        square[4 * t : 4 * t + 4, :] = table[t]
    columns = square[...].T
    rows_iota = lax.broadcasted_iota(jnp.int32, (LANES, LANES), 0)

    def look(profile_row, level):
        pick = rows_iota == profile_row
        return [
            jnp.sum(
                jnp.where(pick, columns[:, 4 * t + level : 4 * t + level + 1], 0.0),
                axis=0,
                keepdims=True,
            )
            for t in range(3)
        ]

    ids[...] = jnp.zeros_like(ids)
    ids[0:1, 0:pol] = policy_profile[...]
    ids[1:2, 0:pol] = policy_owner[...] * prog + policy_slot[...]
    ids[2:3, 0:prog] = program_profile[...]
    own_meta = [(site_owner[...] * pol + site_slot[...]).astype(f32)]
    own_meta += look(ids[0:1, :], 2)
    own_meta += [ids[1:2, :].astype(f32)]
    own_meta += look(ids[2:3, :], 3)
    meta[me] = jnp.concatenate(own_meta, axis=0)

    for b in range(blocks):
        grouping[:, b * LANES : (b + 1) * LANES] = (rows_iota == item_site[b : b + 1, :]).astype(bf16)
        for t, row in enumerate(look(item_profile[b : b + 1, :], 0)):
            square[3 * b + t : 3 * b + t + 1, :] = row
    for t, row in enumerate(look(site_profile[...], 1)):
        square[3 * blocks + t : 3 * blocks + t + 1, :] = row
    flipped = square[...].T
    for t in range(3):
        for b in range(blocks):
            item_terms[t, b * LANES : (b + 1) * LANES, :] = jnp.broadcast_to(
                flipped[:, 3 * b + t : 3 * b + t + 1], (LANES, LANES)
            )
        site_terms[t] = jnp.broadcast_to(
            flipped[:, 3 * blocks + t : 3 * blocks + t + 1], (LANES, LANES)
        )

    pl.semaphore_wait(barrier, n - 1)

    def meta_copy(d, s):
        return pltpu.make_async_remote_copy(
            meta.at[s], meta.at[s], meta_ss.at[d], meta_rs.at[s], device_id={"own": d}
        )

    def site_copy(d, s):
        return pltpu.make_async_remote_copy(
            send.at[d], recv.at[s], site_ss.at[d], site_rs.at[s], device_id={"own": d}
        )

    def policy_copy(d, s):
        return pltpu.make_async_remote_copy(
            losses.at[pl.ds(pl.multiple_of(d * pol, pol), pol), :],
            policy_out.at[:, pl.ds(pl.multiple_of(s * width, width), width)],
            pol_ss.at[d],
            pol_rs.at[s],
            device_id={"own": d},
        )

    def program_copy(d, s):
        return pltpu.make_async_remote_copy(
            program_send.at[d],
            program_out.at[:, pl.ds(pl.multiple_of(s * width, width), width)],
            prog_ss.at[d],
            prog_rs.at[s],
            device_id={"own": d},
        )

    def others(fn):
        def step(k, c):
            fn(lax.rem(me + k, n))
            return c

        lax.fori_loop(1, n, step, 0)

    others(lambda d: meta_copy(d, me).start())

    def sites_step(i, c):
        load(i).wait()
        g = lax.rem(mine + half + i, groups)
        spread = [jnp.concatenate([item_terms[t]] * (wide // LANES), axis=1) for t in range(3)]
        covered = terms(chunks[i].astype(f32), *spread).astype(bf16)
        gross = jnp.dot(grouping[...], covered, preferred_element_type=f32)
        site_spread = [jnp.concatenate([site_terms[t]] * (wide // LANES), axis=1) for t in range(3)]
        net = terms(gross, *site_spread).astype(bf16)
        for j in range(2):
            d = 2 * g + j
            piece = net[:, j * width : (j + 1) * width]

            @pl.when(d == me)
            def _():
                recv[me] = piece

            @pl.when(d != me)
            def _():
                send[d] = piece
                site_copy(d, me).start()

        return c

    lax.fori_loop(0, groups, sites_step, 0)

    others(lambda s: meta_copy(me, s).wait_recv())

    meta_flat = meta[...].reshape(n * META, LANES)
    turned = meta_flat.T
    for o in range(n):
        for t in range(3):
            lane = o * META + 1 + t
            policy_terms[t, o * pol : (o + 1) * pol, :] = jnp.broadcast_to(
                turned[0:pol, lane : lane + 1], (pol, LANES)
            )
            lane = o * META + 5 + t
            program_terms[o, t] = jnp.broadcast_to(turned[0:prog, lane : lane + 1], (prog, LANES))

    policy_iota = lax.broadcasted_iota(jnp.int32, (n * pol, sites), 0).astype(f32)
    order = [0]
    for k in range(1, half + 1):
        order += [k] if k == groups - k else [k, groups - k]
    acc[...] = jnp.zeros_like(acc)

    for k in order:
        g = lax.rem(mine + k, groups)
        for j in range(2):
            s = 2 * g + j

            @pl.when(s != me)
            def _():
                site_copy(me, s).wait_recv()

        pick = jnp.concatenate(
            [(policy_iota == meta[2 * g + j][0:1, :]).astype(bf16) for j in range(2)], axis=1
        )
        values = recv[pl.ds(2 * g, 2)].reshape(2 * sites, width)
        acc[...] += jnp.dot(pick, values, preferred_element_type=f32)

    def policy_step(i, c):
        d = lax.rem(me + n // 2 + i, n)
        at = pl.ds(pl.multiple_of(d * pol, pol), pol)
        spread = [
            jnp.concatenate([policy_terms[t, at, :]] * (width // LANES), axis=1) for t in range(3)
        ]
        losses[at, :] = terms(acc[at, :], *spread).astype(bf16)

        @pl.when(d != me)
        def _():
            policy_copy(d, me).start()

        return c

    lax.fori_loop(0, n, policy_step, 0)
    own_policy = pltpu.make_async_copy(
        losses.at[pl.ds(pl.multiple_of(me * pol, pol), pol), :],
        policy_out.at[:, pl.ds(pl.multiple_of(me * width, width), width)],
        pol_rs.at[me],
    )
    own_policy.start()

    program_iota = lax.broadcasted_iota(jnp.int32, (n * prog, pol), 0).astype(f32)
    marks = [
        (program_iota == meta_flat[o * META + 4 : o * META + 5, 0:pol]).astype(bf16)
        for o in range(n)
    ]
    program_gross = jnp.dot(jnp.concatenate(marks, axis=1), losses[...], preferred_element_type=f32)
    for o in range(n):
        spread = [
            jnp.concatenate([program_terms[o, t]] * (width // LANES), axis=1) for t in range(3)
        ]
        program_send[o] = terms(program_gross[o * prog : (o + 1) * prog, :], *spread)
    others(lambda d: program_copy(d, me).start())
    own_program = pltpu.make_async_copy(
        program_send.at[me],
        program_out.at[:, pl.ds(pl.multiple_of(me * width, width), width)],
        prog_rs.at[me],
    )
    own_program.start()

    def finish(d):
        meta_copy(d, me).wait_send()
        site_copy(d, me).wait_send()
        policy_copy(d, me).wait_send()
        program_copy(d, me).wait_send()
        policy_copy(me, d).wait_recv()
        program_copy(me, d).wait_recv()

    others(finish)
    own_policy.wait()
    own_program.wait()


def exchange(
    ground_up,
    item_site,
    item_profile,
    site_owner,
    site_slot,
    site_profile,
    policy_owner,
    policy_slot,
    policy_profile,
    program_profile,
    term_table,
):
    n = lax.axis_size("own")
    items, cols = ground_up.shape
    sites = site_profile.shape[0]
    pol = policy_profile.shape[0]
    prog = program_profile.shape[0]
    width = cols // n

    def row(v):
        return v.reshape(-1, min(v.size, LANES))

    inputs = [
        row(v)
        for v in (
            item_site,
            item_profile,
            site_owner,
            site_slot,
            site_profile,
            policy_owner,
            policy_slot,
            policy_profile,
            program_profile,
        )
    ] + [term_table.transpose(1, 0, 2)]
    vmemspec = pl.BlockSpec(memory_space=pltpu.VMEM)
    anyspec = pl.BlockSpec(memory_space=pl.ANY)
    dma = pltpu.SemaphoreType.DMA
    return pl.pallas_call(
        functools.partial(kernel, n, pol, prog),
        out_shape=(
            pltpu.VMEM((pol, cols), bf16),
            pltpu.VMEM((prog, cols), f32),
        ),
        in_specs=[anyspec] * (1 + SMALL),
        out_specs=(vmemspec, vmemspec),
        scratch_shapes=[pltpu.VMEM(v.shape, v.dtype) for v in inputs]
        + [
            pltpu.VMEM((n // 2, items, 2 * width), bf16),
            pltpu.VMEM((8, LANES), jnp.int32),
            pltpu.VMEM((LANES, LANES), f32),
            pltpu.VMEM((3, items, LANES), f32),
            pltpu.VMEM((3, sites, LANES), f32),
            pltpu.VMEM((3, n * pol, LANES), f32),
            pltpu.VMEM((n, 3, prog, LANES), f32),
            pltpu.VMEM((sites, items), bf16),
            pltpu.VMEM((n, META, LANES), f32),
            pltpu.VMEM((n, sites, width), bf16),
            pltpu.VMEM((n, sites, width), bf16),
            pltpu.VMEM((n * pol, width), f32),
            pltpu.VMEM((n * pol, width), bf16),
            pltpu.VMEM((n, prog, width), f32),
            dma((SMALL,)),
            dma((n // 2,)),
        ]
        + [dma((n,))] * 8,
        compiler_params=pltpu.CompilerParams(collective_id=0, has_side_effects=True),
        name="loss_terms",
    )(ground_up, *inputs)


def apply_terms(gross_loss, terms_table, tier_index, profile):
    profile_iota = jnp.arange(terms_table.shape[2], dtype=jnp.int32)
    picker = profile[:, None] == profile_iota[None, :]
    deduct = jnp.sum(jnp.where(picker, terms_table[tier_index, 0][None, :], 0.0), axis=1)[:, None]
    ceiling = jnp.sum(jnp.where(picker, terms_table[tier_index, 1][None, :], 0.0), axis=1)[:, None]
    portion = jnp.sum(jnp.where(picker, terms_table[tier_index, 2][None, :], 0.0), axis=1)[:, None]
    return portion * jnp.minimum(jnp.maximum(gross_loss - deduct, 0.0), ceiling)


def pack_rows(values, target_dev, inner_slot, owners, capacity):
    member = (target_dev[:, None] == jnp.arange(owners, dtype=jnp.int32)[None, :]).astype(jnp.int32)
    before = jnp.cumsum(member, axis=0) - member
    position = jnp.sum(before * member, axis=1)
    target = target_dev * capacity + position
    placer = jnp.arange(owners * capacity, dtype=jnp.int32)[:, None] == target[None, :]
    packed = jnp.dot(
        placer.astype(jnp.bfloat16), values, preferred_element_type=jnp.float32
    ).astype(jnp.bfloat16)
    labels = jnp.sum(jnp.where(placer, (inner_slot + 1)[None, :], 0), axis=1) - 1
    return (
        packed.reshape(owners, capacity, values.shape[1]),
        labels.astype(jnp.bfloat16).reshape(owners, capacity),
    )


def sum_rows(received, labels, slot_count):
    flattened = received.reshape(-1, received.shape[2])
    slot_marks = labels.reshape(-1).astype(jnp.int32)
    picker = (jnp.arange(slot_count, dtype=jnp.int32)[:, None] == slot_marks[None, :]).astype(
        jnp.bfloat16
    )
    return jnp.dot(picker, flattened, preferred_element_type=jnp.float32)


def shards(
    ground_up,
    item_site,
    item_profile,
    site_owner,
    site_slot,
    site_profile,
    policy_owner,
    policy_slot,
    policy_profile,
    program_profile,
    term_table,
):
    owners = lax.axis_size("own")
    covered = apply_terms(ground_up.astype(jnp.float32), term_table, 0, item_profile).astype(
        jnp.bfloat16
    )
    site_total = site_profile.shape[0]
    grouping = (jnp.arange(site_total, dtype=jnp.int32)[:, None] == item_site[None, :]).astype(
        jnp.bfloat16
    )
    site_gross = jnp.dot(grouping, covered, preferred_element_type=jnp.float32)
    site_net = apply_terms(site_gross, term_table, 1, site_profile).astype(jnp.bfloat16)
    capacity = 2 * site_total // owners
    packed, labels = pack_rows(site_net, site_owner[:, 0], site_slot, owners, capacity)
    arrived, arrived_labels = (
        lax.all_to_all(packed, "own", split_axis=0, concat_axis=0, tiled=True),
        lax.all_to_all(labels, "own", split_axis=0, concat_axis=0, tiled=True),
    )
    policy_total = policy_profile.shape[0]
    policy_gross = sum_rows(arrived, arrived_labels, policy_total)
    policy_loss = apply_terms(policy_gross, term_table, 2, policy_profile).astype(jnp.bfloat16)
    program_total = program_profile.shape[0]
    program_capacity = 3 * policy_total // owners
    sent_rows, sent_labels = pack_rows(
        policy_loss, policy_owner[:, 0], policy_slot, owners, program_capacity
    )
    got_rows, got_labels = (
        lax.all_to_all(sent_rows, "own", split_axis=0, concat_axis=0, tiled=True),
        lax.all_to_all(sent_labels, "own", split_axis=0, concat_axis=0, tiled=True),
    )
    program_gross = sum_rows(got_rows, got_labels, program_total)
    program_loss = apply_terms(program_gross, term_table, 3, program_profile)
    return (policy_loss, program_loss)


def solution(mesh):
    placed = (
        P("own", "ev"),
        P("own"),
        P("own"),
        P("own", None),
        P("own"),
        P("own"),
        P("own", None),
        P("own"),
        P("own"),
        P("own"),
        P(),
    )

    def body(ground_up, item_site, item_profile, *rest):
        n = lax.axis_size("own")
        items, cols = ground_up.shape
        sites, pol = rest[2].shape[0], rest[5].shape[0]
        prog = rest[6].shape[0]
        fits = cols % (n * LANES) == 0 and items % LANES == 0 and sites == LANES
        fits = fits and pol <= LANES and pol % 16 == 0 and prog <= 8
        fits = fits and n % 4 == 0 and n * META <= LANES and 3 * items <= LANES * (LANES - 3)
        return (exchange if fits else shards)(ground_up, item_site, item_profile, *rest)

    return jax.shard_map(
        body,
        mesh=mesh,
        in_specs=placed,
        out_specs=(P("own", "ev"), P("own", "ev")),
        check_vma=False,
    )
```

```python
import functools

import jax
import jax.numpy as jnp
from jax import lax
from jax.experimental import pallas as pl
from jax.experimental.pallas import tpu as pltpu
from jax.sharding import PartitionSpec as P

LANES = 128
SMALL = 10
f32 = jnp.float32
bf16 = jnp.bfloat16


def terms(x, deduct, ceiling, portion):
    return portion * jnp.minimum(jnp.maximum(x - deduct, 0.0), ceiling)


def across(me, k, n):
    d, bit = 0, 1
    while bit < n:
        d = d + bit * lax.rem(lax.div(me, bit) + (k // bit) % 2, 2)
        bit *= 2
    return d


def route(n):
    return [k for i in range(n // 2) for k in (n // 2 + i, i) if k]


def kernel(
    n,
    pol,
    prog,
    ground,
    *refs,
):
    small_in, refs = refs[:SMALL], refs[SMALL:]
    policy_out, program_out = refs[:2]
    small, refs = refs[2 : 2 + SMALL], refs[2 + SMALL :]
    (
        chunks,
        ids,
        square,
        item_terms,
        site_terms,
        policy_terms,
        program_terms,
        grouping,
        meta,
        send,
        recv,
        acc,
        losses,
        program_send,
        small_sem,
        load_sem,
        meta_ss,
        meta_rs,
        site_ss,
        site_rs,
        pol_ss,
        pol_rs,
        prog_ss,
        prog_rs,
    ) = refs
    me = lax.axis_index("own")
    groups = n // 2
    mine = me // 2
    half = groups // 2
    items = ground.shape[0]
    blocks = items // LANES
    sites = send.shape[1]
    width = send.shape[2]
    wide = 2 * width

    barrier = pltpu.get_barrier_semaphore()

    def greet(k, c):
        pl.semaphore_signal(barrier, inc=1, device_id={"own": lax.rem(me + k, n)})
        return c

    lax.fori_loop(1, n, greet, 0)

    def fetch(i):
        return pltpu.make_async_copy(small_in[i], small[i], small_sem.at[i])

    for i in range(SMALL):
        fetch(i).start()

    def load(i):
        g = lax.rem(mine + half + i, groups)
        return pltpu.make_async_copy(
            ground.at[:, pl.ds(pl.multiple_of(g * wide, wide), wide)],
            chunks.at[i],
            load_sem.at[i],
        )

    def start_load(i, c):
        load(i).start()
        return c

    lax.fori_loop(0, groups, start_load, 0)
    (
        item_site,
        item_profile,
        site_owner,
        site_slot,
        site_profile,
        policy_owner,
        policy_slot,
        policy_profile,
        program_profile,
        table,
    ) = small
    for i in range(SMALL):
        fetch(i).wait()

    square[...] = jnp.zeros_like(square)
    for t in range(3):
        square[4 * t : 4 * t + 4, :] = table[t]
    columns = square[...].T
    rows_iota = lax.broadcasted_iota(jnp.int32, (LANES, LANES), 0)

    def look(profile_row, level):
        pick = rows_iota == profile_row
        return [
            jnp.sum(
                jnp.where(pick, columns[:, 4 * t + level : 4 * t + level + 1], 0.0),
                axis=0,
                keepdims=True,
            )
            for t in range(3)
        ]

    ids[...] = jnp.zeros_like(ids)
    ids[0:1, 0:pol] = policy_profile[...]
    ids[0:1, pol : 2 * pol] = policy_owner[...] * prog + policy_slot[...]
    ids[1:2, 0:prog] = program_profile[...]
    meta[me] = jnp.concatenate([site_owner[...] * pol + site_slot[...], ids[0:1, :]], axis=0)

    for b in range(blocks):
        grouping[:, b * LANES : (b + 1) * LANES] = (rows_iota == item_site[b : b + 1, :]).astype(bf16)
        for t, row in enumerate(look(item_profile[b : b + 1, :], 0)):
            square[3 * b + t : 3 * b + t + 1, :] = row
    for t, row in enumerate(look(site_profile[...], 1)):
        square[3 * blocks + t : 3 * blocks + t + 1, :] = row
    for t, row in enumerate(look(ids[1:2, :], 3)):
        square[3 * blocks + 3 + t : 3 * blocks + 4 + t, :] = row
    flipped = square[...].T
    for t in range(3):
        for b in range(blocks):
            item_terms[t, b * LANES : (b + 1) * LANES, :] = jnp.broadcast_to(
                flipped[:, 3 * b + t : 3 * b + t + 1], (LANES, LANES)
            )
        program_terms[t] = jnp.broadcast_to(
            flipped[0:prog, 3 * blocks + 3 + t : 3 * blocks + 4 + t], (prog, LANES)
        )
        site_terms[t] = jnp.broadcast_to(
            flipped[:, 3 * blocks + t : 3 * blocks + t + 1], (LANES, LANES)
        )

    def meta_copy(d, s):
        return pltpu.make_async_remote_copy(
            meta.at[s], meta.at[s], meta_ss.at[d], meta_rs.at[s], device_id={"own": d}
        )

    def site_copy(d, s):
        return pltpu.make_async_remote_copy(
            send.at[d], recv.at[s], site_ss.at[d], site_rs.at[s], device_id={"own": d}
        )

    def policy_copy(d, s):
        return pltpu.make_async_remote_copy(
            losses.at[pl.ds(pl.multiple_of(d * pol, pol), pol), :],
            policy_out.at[:, pl.ds(pl.multiple_of(s * width, width), width)],
            pol_ss.at[d],
            pol_rs.at[s],
            device_id={"own": d},
        )

    def program_copy(d, s):
        return pltpu.make_async_remote_copy(
            program_send.at[d],
            program_out.at[:, pl.ds(pl.multiple_of(s * width, width), width)],
            prog_ss.at[d],
            prog_rs.at[s],
            device_id={"own": d},
        )

    def others(fn):
        def step(k, c):
            fn(lax.rem(me + k, n))
            return c

        lax.fori_loop(1, n, step, 0)

    def sites_step(i, c):
        load(i).wait()
        g = lax.rem(mine + half + i, groups)
        spread = [jnp.concatenate([item_terms[t]] * (wide // LANES), axis=1) for t in range(3)]
        covered = terms(chunks[i].astype(f32), *spread).astype(bf16)
        gross = jnp.dot(grouping[...], covered, preferred_element_type=f32)
        site_spread = [jnp.concatenate([site_terms[t]] * (wide // LANES), axis=1) for t in range(3)]
        net = terms(gross, *site_spread).astype(bf16)
        for j in range(2):
            d = 2 * g + j
            piece = net[:, j * width : (j + 1) * width]

            @pl.when(d == me)
            def _():
                recv[me] = piece

            @pl.when(d != me)
            def _():
                send[d] = piece

        return c

    lax.fori_loop(0, groups, sites_step, 0)

    pl.semaphore_wait(barrier, n - 1)

    others(lambda d: meta_copy(d, me).start())

    for k in route(n):
        d = across(me, k, n)
        site_copy(d, me).start()

    others(lambda s: meta_copy(me, s).wait_recv())

    for o in range(n):
        for t, row in enumerate(look(meta[o][1:2, :], 2)):
            square[3 * o + t : 3 * o + t + 1, :] = row
    turned = square[...].T
    for o in range(n):
        for t in range(3):
            lane = 3 * o + t
            policy_terms[t, o * pol : (o + 1) * pol, :] = jnp.broadcast_to(
                turned[0:pol, lane : lane + 1], (pol, LANES)
            )

    policy_iota = lax.broadcasted_iota(jnp.int32, (n * pol, sites), 0)
    order = [0]
    for k in range(1, half + 1):
        order += [k] if k == groups - k else [k, groups - k]
    acc[...] = jnp.zeros_like(acc)

    for k in order:
        g = lax.rem(mine + k, groups)
        for j in range(2):
            s = 2 * g + j

            @pl.when(s != me)
            def _():
                site_copy(me, s).wait_recv()

        pick = jnp.concatenate(
            [(policy_iota == meta[2 * g + j][0:1, :]).astype(bf16) for j in range(2)], axis=1
        )
        values = recv[pl.ds(2 * g, 2)].reshape(2 * sites, width)
        acc[...] += jnp.dot(pick, values, preferred_element_type=f32)

    for k in route(n) + [0]:
        d = across(me, k, n)
        at = pl.ds(pl.multiple_of(d * pol, pol), pol)
        spread = [
            jnp.concatenate([policy_terms[t, at, :]] * (width // LANES), axis=1) for t in range(3)
        ]
        losses[at, :] = terms(acc[at, :], *spread).astype(bf16)
        if k:
            policy_copy(d, me).start()
    own_policy = pltpu.make_async_copy(
        losses.at[pl.ds(pl.multiple_of(me * pol, pol), pol), :],
        policy_out.at[:, pl.ds(pl.multiple_of(me * width, width), width)],
        pol_rs.at[me],
    )
    own_policy.start()

    program_iota = lax.broadcasted_iota(jnp.int32, (n * prog, pol), 0)
    marks = [
        (program_iota == meta[o][1:2, pol : 2 * pol]).astype(bf16)
        for o in range(n)
    ]
    program_gross = jnp.dot(jnp.concatenate(marks, axis=1), losses[...], preferred_element_type=f32)
    for o in range(n):
        program_send[o] = program_gross[o * prog : (o + 1) * prog, :]
    for k in route(n):
        program_copy(across(me, k, n), me).start()
    own_program = pltpu.make_async_copy(
        program_send.at[me],
        program_out.at[:, pl.ds(pl.multiple_of(me * width, width), width)],
        prog_rs.at[me],
    )
    own_program.start()

    def finish(d):
        meta_copy(d, me).wait_send()
        site_copy(d, me).wait_send()
        policy_copy(d, me).wait_send()
        program_copy(d, me).wait_send()
        policy_copy(me, d).wait_recv()
        program_copy(me, d).wait_recv()

    others(finish)
    own_policy.wait()
    own_program.wait()
    spread = [jnp.concatenate([program_terms[t]] * (program_out.shape[1] // LANES), axis=1) for t in range(3)]
    program_out[...] = terms(program_out[...], *spread)


def exchange(
    ground_up,
    item_site,
    item_profile,
    site_owner,
    site_slot,
    site_profile,
    policy_owner,
    policy_slot,
    policy_profile,
    program_profile,
    term_table,
):
    n = lax.axis_size("own")
    items, cols = ground_up.shape
    sites = site_profile.shape[0]
    pol = policy_profile.shape[0]
    prog = program_profile.shape[0]
    width = cols // n

    def row(v):
        return v.reshape(-1, min(v.size, LANES))

    inputs = [
        row(v)
        for v in (
            item_site,
            item_profile,
            site_owner,
            site_slot,
            site_profile,
            policy_owner,
            policy_slot,
            policy_profile,
            program_profile,
        )
    ] + [term_table.transpose(1, 0, 2)]
    vmemspec = pl.BlockSpec(memory_space=pltpu.VMEM)
    anyspec = pl.BlockSpec(memory_space=pl.ANY)
    dma = pltpu.SemaphoreType.DMA
    return pl.pallas_call(
        functools.partial(kernel, n, pol, prog),
        out_shape=(
            pltpu.VMEM((pol, cols), bf16),
            pltpu.VMEM((prog, cols), f32),
        ),
        in_specs=[anyspec] * (1 + SMALL),
        out_specs=(vmemspec, vmemspec),
        scratch_shapes=[pltpu.VMEM(v.shape, v.dtype) for v in inputs]
        + [
            pltpu.VMEM((n // 2, items, 2 * width), bf16),
            pltpu.VMEM((8, LANES), jnp.int32),
            pltpu.VMEM((LANES, LANES), f32),
            pltpu.VMEM((3, items, LANES), f32),
            pltpu.VMEM((3, sites, LANES), f32),
            pltpu.VMEM((3, n * pol, LANES), f32),
            pltpu.VMEM((3, prog, LANES), f32),
            pltpu.VMEM((sites, items), bf16),
            pltpu.VMEM((n, 2, LANES), jnp.int32),
            pltpu.VMEM((n, sites, width), bf16),
            pltpu.VMEM((n, sites, width), bf16),
            pltpu.VMEM((n * pol, width), f32),
            pltpu.VMEM((n * pol, width), bf16),
            pltpu.VMEM((n, prog, width), f32),
            dma((SMALL,)),
            dma((n // 2,)),
        ]
        + [dma((n,))] * 8,
        compiler_params=pltpu.CompilerParams(collective_id=0, has_side_effects=True),
        name="loss_terms",
    )(ground_up, *inputs)


def apply_terms(gross_loss, terms_table, tier_index, profile):
    profile_iota = jnp.arange(terms_table.shape[2], dtype=jnp.int32)
    picker = profile[:, None] == profile_iota[None, :]
    deduct = jnp.sum(jnp.where(picker, terms_table[tier_index, 0][None, :], 0.0), axis=1)[:, None]
    ceiling = jnp.sum(jnp.where(picker, terms_table[tier_index, 1][None, :], 0.0), axis=1)[:, None]
    portion = jnp.sum(jnp.where(picker, terms_table[tier_index, 2][None, :], 0.0), axis=1)[:, None]
    return portion * jnp.minimum(jnp.maximum(gross_loss - deduct, 0.0), ceiling)


def pack_rows(values, target_dev, inner_slot, owners, capacity):
    member = (target_dev[:, None] == jnp.arange(owners, dtype=jnp.int32)[None, :]).astype(jnp.int32)
    before = jnp.cumsum(member, axis=0) - member
    position = jnp.sum(before * member, axis=1)
    target = target_dev * capacity + position
    placer = jnp.arange(owners * capacity, dtype=jnp.int32)[:, None] == target[None, :]
    packed = jnp.dot(
        placer.astype(jnp.bfloat16), values, preferred_element_type=jnp.float32
    ).astype(jnp.bfloat16)
    labels = jnp.sum(jnp.where(placer, (inner_slot + 1)[None, :], 0), axis=1) - 1
    return (
        packed.reshape(owners, capacity, values.shape[1]),
        labels.astype(jnp.bfloat16).reshape(owners, capacity),
    )


def sum_rows(received, labels, slot_count):
    flattened = received.reshape(-1, received.shape[2])
    slot_marks = labels.reshape(-1).astype(jnp.int32)
    picker = (jnp.arange(slot_count, dtype=jnp.int32)[:, None] == slot_marks[None, :]).astype(
        jnp.bfloat16
    )
    return jnp.dot(picker, flattened, preferred_element_type=jnp.float32)


def shards(
    ground_up,
    item_site,
    item_profile,
    site_owner,
    site_slot,
    site_profile,
    policy_owner,
    policy_slot,
    policy_profile,
    program_profile,
    term_table,
):
    owners = lax.axis_size("own")
    covered = apply_terms(ground_up.astype(jnp.float32), term_table, 0, item_profile).astype(
        jnp.bfloat16
    )
    site_total = site_profile.shape[0]
    grouping = (jnp.arange(site_total, dtype=jnp.int32)[:, None] == item_site[None, :]).astype(
        jnp.bfloat16
    )
    site_gross = jnp.dot(grouping, covered, preferred_element_type=jnp.float32)
    site_net = apply_terms(site_gross, term_table, 1, site_profile).astype(jnp.bfloat16)
    capacity = 2 * site_total // owners
    packed, labels = pack_rows(site_net, site_owner[:, 0], site_slot, owners, capacity)
    arrived, arrived_labels = (
        lax.all_to_all(packed, "own", split_axis=0, concat_axis=0, tiled=True),
        lax.all_to_all(labels, "own", split_axis=0, concat_axis=0, tiled=True),
    )
    policy_total = policy_profile.shape[0]
    policy_gross = sum_rows(arrived, arrived_labels, policy_total)
    policy_loss = apply_terms(policy_gross, term_table, 2, policy_profile).astype(jnp.bfloat16)
    program_total = program_profile.shape[0]
    program_capacity = 3 * policy_total // owners
    sent_rows, sent_labels = pack_rows(
        policy_loss, policy_owner[:, 0], policy_slot, owners, program_capacity
    )
    got_rows, got_labels = (
        lax.all_to_all(sent_rows, "own", split_axis=0, concat_axis=0, tiled=True),
        lax.all_to_all(sent_labels, "own", split_axis=0, concat_axis=0, tiled=True),
    )
    program_gross = sum_rows(got_rows, got_labels, program_total)
    program_loss = apply_terms(program_gross, term_table, 3, program_profile)
    return (policy_loss, program_loss)


def solution(mesh):
    placed = (
        P("own", "ev"),
        P("own"),
        P("own"),
        P("own", None),
        P("own"),
        P("own"),
        P("own", None),
        P("own"),
        P("own"),
        P("own"),
        P(),
    )

    def body(ground_up, item_site, item_profile, *rest):
        n = lax.axis_size("own")
        items, cols = ground_up.shape
        sites, pol = rest[2].shape[0], rest[5].shape[0]
        prog = rest[6].shape[0]
        fits = cols % (n * LANES) == 0 and items % LANES == 0 and sites == LANES
        fits = fits and 2 * pol <= LANES and pol % 16 == 0 and prog <= 8
        fits = fits and n % 4 == 0 and n & (n - 1) == 0 and 3 * n <= LANES and 3 * items <= LANES * (LANES - 6)
        return (exchange if fits else shards)(ground_up, item_site, item_profile, *rest)

    return jax.shard_map(
        body,
        mesh=mesh,
        in_specs=placed,
        out_specs=(P("own", "ev"), P("own", "ev")),
        check_vma=False,
    )
```

```python
import functools

import jax
import jax.numpy as jnp
from jax import lax
from jax.experimental import pallas as pl
from jax.experimental.pallas import tpu as pltpu
from jax.sharding import PartitionSpec as P

LANES = 128
SMALL = 10
f32 = jnp.float32
bf16 = jnp.bfloat16


def terms(x, deduct, ceiling, portion):
    return portion * jnp.minimum(jnp.maximum(x - deduct, 0.0), ceiling)


def across(me, k, n):
    d, bit = 0, 1
    while bit < n:
        d = d + bit * lax.rem(lax.div(me, bit) + (k // bit) % 2, 2)
        bit *= 2
    return d


def route(n):
    return [k for i in range(n // 2) for k in (n // 2 + i, i) if k]


def kernel(
    n,
    pol,
    prog,
    ground,
    *refs,
):
    small_in, refs = refs[:SMALL], refs[SMALL:]
    policy_out, program_out = refs[:2]
    small, refs = refs[2 : 2 + SMALL], refs[2 + SMALL :]
    (
        chunks,
        ids,
        square,
        item_terms,
        site_terms,
        policy_terms,
        program_terms,
        grouping,
        meta,
        send,
        recv,
        acc,
        losses,
        program_send,
        marks,
        picks,
        small_sem,
        load_sem,
        meta_ss,
        meta_rs,
        site_ss,
        site_rs,
        pol_ss,
        pol_rs,
        prog_ss,
        prog_rs,
    ) = refs
    me = lax.axis_index("own")
    groups = n // 2
    mine = me // 2
    half = groups // 2
    items = ground.shape[0]
    blocks = items // LANES
    sites = send.shape[1]
    width = send.shape[2]
    wide = 2 * width

    barrier = pltpu.get_barrier_semaphore()

    def greet(k, c):
        pl.semaphore_signal(barrier, inc=1, device_id={"own": lax.rem(me + k, n)})
        return c

    lax.fori_loop(1, n, greet, 0)

    def fetch(i):
        return pltpu.make_async_copy(small_in[i], small[i], small_sem.at[i])

    for i in range(SMALL):
        fetch(i).start()

    def load(i):
        g = lax.rem(mine + half + i, groups)
        return pltpu.make_async_copy(
            ground.at[:, pl.ds(pl.multiple_of(g * wide, wide), wide)],
            chunks.at[i],
            load_sem.at[i],
        )

    def start_load(i, c):
        load(i).start()
        return c

    lax.fori_loop(0, groups, start_load, 0)
    (
        item_site,
        item_profile,
        site_owner,
        site_slot,
        site_profile,
        policy_owner,
        policy_slot,
        policy_profile,
        program_profile,
        table,
    ) = small
    for i in range(SMALL):
        fetch(i).wait()

    square[...] = jnp.zeros_like(square)
    for t in range(3):
        square[4 * t : 4 * t + 4, :] = table[t]
    columns = square[...].T
    rows_iota = lax.broadcasted_iota(jnp.int32, (LANES, LANES), 0)

    def look(profile_row, level):
        pick = rows_iota == profile_row
        return [
            jnp.sum(
                jnp.where(pick, columns[:, 4 * t + level : 4 * t + level + 1], 0.0),
                axis=0,
                keepdims=True,
            )
            for t in range(3)
        ]

    ids[...] = jnp.zeros_like(ids)
    ids[0:1, 0:pol] = policy_profile[...]
    ids[0:1, pol : 2 * pol] = policy_owner[...] * prog + policy_slot[...]
    ids[1:2, 0:prog] = program_profile[...]
    meta[me] = jnp.concatenate([site_owner[...] * pol + site_slot[...], ids[0:1, :]], axis=0)

    for b in range(blocks):
        grouping[:, b * LANES : (b + 1) * LANES] = (rows_iota == item_site[b : b + 1, :]).astype(bf16)
        for t, row in enumerate(look(item_profile[b : b + 1, :], 0)):
            square[3 * b + t : 3 * b + t + 1, :] = row
    for t, row in enumerate(look(site_profile[...], 1)):
        square[3 * blocks + t : 3 * blocks + t + 1, :] = row
    for t, row in enumerate(look(ids[1:2, :], 3)):
        square[3 * blocks + 3 + t : 3 * blocks + 4 + t, :] = row
    flipped = square[...].T
    for t in range(3):
        for b in range(blocks):
            item_terms[t, b * LANES : (b + 1) * LANES, :] = jnp.broadcast_to(
                flipped[:, 3 * b + t : 3 * b + t + 1], (LANES, LANES)
            )
        program_terms[t] = jnp.broadcast_to(
            flipped[0:prog, 3 * blocks + 3 + t : 3 * blocks + 4 + t], (prog, LANES)
        )
        site_terms[t] = jnp.broadcast_to(
            flipped[:, 3 * blocks + t : 3 * blocks + t + 1], (LANES, LANES)
        )

    def meta_copy(d, s):
        return pltpu.make_async_remote_copy(
            meta.at[s], meta.at[s], meta_ss.at[d], meta_rs.at[s], device_id={"own": d}
        )

    def site_copy(d, s):
        return pltpu.make_async_remote_copy(
            send.at[d], recv.at[s], site_ss.at[d], site_rs.at[s], device_id={"own": d}
        )

    def policy_copy(d, s):
        return pltpu.make_async_remote_copy(
            losses.at[pl.ds(pl.multiple_of(d * pol, pol), pol), :],
            policy_out.at[:, pl.ds(pl.multiple_of(s * width, width), width)],
            pol_ss.at[d],
            pol_rs.at[s],
            device_id={"own": d},
        )

    def program_copy(d, s):
        return pltpu.make_async_remote_copy(
            program_send.at[d],
            program_out.at[:, pl.ds(pl.multiple_of(s * width, width), width)],
            prog_ss.at[d],
            prog_rs.at[s],
            device_id={"own": d},
        )

    def others(fn):
        def step(k, c):
            fn(lax.rem(me + k, n))
            return c

        lax.fori_loop(1, n, step, 0)

    def sites_step(i, c):
        load(i).wait()
        g = lax.rem(mine + half + i, groups)
        spread = [jnp.concatenate([item_terms[t]] * (wide // LANES), axis=1) for t in range(3)]
        covered = terms(chunks[i].astype(f32), *spread).astype(bf16)
        gross = jnp.dot(grouping[...], covered, preferred_element_type=f32)
        site_spread = [jnp.concatenate([site_terms[t]] * (wide // LANES), axis=1) for t in range(3)]
        net = terms(gross, *site_spread).astype(bf16)
        for j in range(2):
            d = 2 * g + j
            piece = net[:, j * width : (j + 1) * width]

            @pl.when(d == me)
            def _():
                recv[me] = piece

            @pl.when(d != me)
            def _():
                send[d] = piece

        return c

    lax.fori_loop(0, groups, sites_step, 0)

    pl.semaphore_wait(barrier, n - 1)

    others(lambda d: meta_copy(d, me).start())

    for k in route(n):
        d = across(me, k, n)
        site_copy(d, me).start()

    others(lambda s: meta_copy(me, s).wait_recv())

    for o in range(n):
        for t, row in enumerate(look(meta[o][1:2, :], 2)):
            square[3 * o + t : 3 * o + t + 1, :] = row
    turned = square[...].T
    for o in range(n):
        for t in range(3):
            lane = 3 * o + t
            policy_terms[t, o * pol : (o + 1) * pol, :] = jnp.broadcast_to(
                turned[0:pol, lane : lane + 1], (pol, LANES)
            )

    policy_iota = lax.broadcasted_iota(jnp.int32, (n * pol, sites), 0)
    program_iota = lax.broadcasted_iota(jnp.int32, (n * prog, pol), 0)
    marks[...] = jnp.concatenate(
        [(program_iota == meta[o][1:2, pol : 2 * pol]).astype(bf16) for o in range(n)], axis=1
    )
    for k in range(groups):
        g = across(mine, k, groups)
        picks[k] = jnp.concatenate(
            [(policy_iota == meta[2 * g + j][0:1, :]).astype(bf16) for j in range(2)], axis=1
        )
    acc[...] = jnp.zeros_like(acc)

    for k in range(groups):
        g = across(mine, k, groups)
        for j in range(2):
            s = 2 * g + j

            @pl.when(s != me)
            def _():
                site_copy(me, s).wait_recv()

        values = recv[pl.ds(2 * g, 2)].reshape(2 * sites, width)
        acc[...] += jnp.dot(picks[k], values, preferred_element_type=f32)

    for k in route(n) + [0]:
        d = across(me, k, n)
        at = pl.ds(pl.multiple_of(d * pol, pol), pol)
        spread = [
            jnp.concatenate([policy_terms[t, at, :]] * (width // LANES), axis=1) for t in range(3)
        ]
        losses[at, :] = terms(acc[at, :], *spread).astype(bf16)
        if k:
            policy_copy(d, me).start()
    own_policy = pltpu.make_async_copy(
        losses.at[pl.ds(pl.multiple_of(me * pol, pol), pol), :],
        policy_out.at[:, pl.ds(pl.multiple_of(me * width, width), width)],
        pol_rs.at[me],
    )
    own_policy.start()

    program_gross = jnp.dot(marks[...], losses[...], preferred_element_type=f32)
    for o in range(n):
        program_send[o] = program_gross[o * prog : (o + 1) * prog, :]
    for k in route(n):
        program_copy(across(me, k, n), me).start()
    own_program = pltpu.make_async_copy(
        program_send.at[me],
        program_out.at[:, pl.ds(pl.multiple_of(me * width, width), width)],
        prog_rs.at[me],
    )
    own_program.start()

    def finish(d):
        meta_copy(d, me).wait_send()
        site_copy(d, me).wait_send()
        policy_copy(d, me).wait_send()
        program_copy(d, me).wait_send()
        policy_copy(me, d).wait_recv()
        program_copy(me, d).wait_recv()

    others(finish)
    own_policy.wait()
    own_program.wait()
    spread = [jnp.concatenate([program_terms[t]] * (program_out.shape[1] // LANES), axis=1) for t in range(3)]
    program_out[...] = terms(program_out[...], *spread)


def exchange(
    ground_up,
    item_site,
    item_profile,
    site_owner,
    site_slot,
    site_profile,
    policy_owner,
    policy_slot,
    policy_profile,
    program_profile,
    term_table,
):
    n = lax.axis_size("own")
    items, cols = ground_up.shape
    sites = site_profile.shape[0]
    pol = policy_profile.shape[0]
    prog = program_profile.shape[0]
    width = cols // n

    def row(v):
        return v.reshape(-1, min(v.size, LANES))

    inputs = [
        row(v)
        for v in (
            item_site,
            item_profile,
            site_owner,
            site_slot,
            site_profile,
            policy_owner,
            policy_slot,
            policy_profile,
            program_profile,
        )
    ] + [term_table.transpose(1, 0, 2)]
    vmemspec = pl.BlockSpec(memory_space=pltpu.VMEM)
    anyspec = pl.BlockSpec(memory_space=pl.ANY)
    dma = pltpu.SemaphoreType.DMA
    return pl.pallas_call(
        functools.partial(kernel, n, pol, prog),
        out_shape=(
            pltpu.VMEM((pol, cols), bf16),
            pltpu.VMEM((prog, cols), f32),
        ),
        in_specs=[anyspec] * (1 + SMALL),
        out_specs=(vmemspec, vmemspec),
        scratch_shapes=[pltpu.VMEM(v.shape, v.dtype) for v in inputs]
        + [
            pltpu.VMEM((n // 2, items, 2 * width), bf16),
            pltpu.VMEM((8, LANES), jnp.int32),
            pltpu.VMEM((LANES, LANES), f32),
            pltpu.VMEM((3, items, LANES), f32),
            pltpu.VMEM((3, sites, LANES), f32),
            pltpu.VMEM((3, n * pol, LANES), f32),
            pltpu.VMEM((3, prog, LANES), f32),
            pltpu.VMEM((sites, items), bf16),
            pltpu.VMEM((n, 2, LANES), jnp.int32),
            pltpu.VMEM((n, sites, width), bf16),
            pltpu.VMEM((n, sites, width), bf16),
            pltpu.VMEM((n * pol, width), f32),
            pltpu.VMEM((n * pol, width), bf16),
            pltpu.VMEM((n, prog, width), f32),
            pltpu.VMEM((n * prog, n * pol), bf16),
            pltpu.VMEM((n // 2, n * pol, 2 * sites), bf16),
            dma((SMALL,)),
            dma((n // 2,)),
        ]
        + [dma((n,))] * 8,
        compiler_params=pltpu.CompilerParams(collective_id=0, has_side_effects=True),
        name="loss_terms",
    )(ground_up, *inputs)


def apply_terms(gross_loss, terms_table, tier_index, profile):
    profile_iota = jnp.arange(terms_table.shape[2], dtype=jnp.int32)
    picker = profile[:, None] == profile_iota[None, :]
    deduct = jnp.sum(jnp.where(picker, terms_table[tier_index, 0][None, :], 0.0), axis=1)[:, None]
    ceiling = jnp.sum(jnp.where(picker, terms_table[tier_index, 1][None, :], 0.0), axis=1)[:, None]
    portion = jnp.sum(jnp.where(picker, terms_table[tier_index, 2][None, :], 0.0), axis=1)[:, None]
    return portion * jnp.minimum(jnp.maximum(gross_loss - deduct, 0.0), ceiling)


def pack_rows(values, target_dev, inner_slot, owners, capacity):
    member = (target_dev[:, None] == jnp.arange(owners, dtype=jnp.int32)[None, :]).astype(jnp.int32)
    before = jnp.cumsum(member, axis=0) - member
    position = jnp.sum(before * member, axis=1)
    target = target_dev * capacity + position
    placer = jnp.arange(owners * capacity, dtype=jnp.int32)[:, None] == target[None, :]
    packed = jnp.dot(
        placer.astype(jnp.bfloat16), values, preferred_element_type=jnp.float32
    ).astype(jnp.bfloat16)
    labels = jnp.sum(jnp.where(placer, (inner_slot + 1)[None, :], 0), axis=1) - 1
    return (
        packed.reshape(owners, capacity, values.shape[1]),
        labels.astype(jnp.bfloat16).reshape(owners, capacity),
    )


def sum_rows(received, labels, slot_count):
    flattened = received.reshape(-1, received.shape[2])
    slot_marks = labels.reshape(-1).astype(jnp.int32)
    picker = (jnp.arange(slot_count, dtype=jnp.int32)[:, None] == slot_marks[None, :]).astype(
        jnp.bfloat16
    )
    return jnp.dot(picker, flattened, preferred_element_type=jnp.float32)


def shards(
    ground_up,
    item_site,
    item_profile,
    site_owner,
    site_slot,
    site_profile,
    policy_owner,
    policy_slot,
    policy_profile,
    program_profile,
    term_table,
):
    owners = lax.axis_size("own")
    covered = apply_terms(ground_up.astype(jnp.float32), term_table, 0, item_profile).astype(
        jnp.bfloat16
    )
    site_total = site_profile.shape[0]
    grouping = (jnp.arange(site_total, dtype=jnp.int32)[:, None] == item_site[None, :]).astype(
        jnp.bfloat16
    )
    site_gross = jnp.dot(grouping, covered, preferred_element_type=jnp.float32)
    site_net = apply_terms(site_gross, term_table, 1, site_profile).astype(jnp.bfloat16)
    capacity = 2 * site_total // owners
    packed, labels = pack_rows(site_net, site_owner[:, 0], site_slot, owners, capacity)
    arrived, arrived_labels = (
        lax.all_to_all(packed, "own", split_axis=0, concat_axis=0, tiled=True),
        lax.all_to_all(labels, "own", split_axis=0, concat_axis=0, tiled=True),
    )
    policy_total = policy_profile.shape[0]
    policy_gross = sum_rows(arrived, arrived_labels, policy_total)
    policy_loss = apply_terms(policy_gross, term_table, 2, policy_profile).astype(jnp.bfloat16)
    program_total = program_profile.shape[0]
    program_capacity = 3 * policy_total // owners
    sent_rows, sent_labels = pack_rows(
        policy_loss, policy_owner[:, 0], policy_slot, owners, program_capacity
    )
    got_rows, got_labels = (
        lax.all_to_all(sent_rows, "own", split_axis=0, concat_axis=0, tiled=True),
        lax.all_to_all(sent_labels, "own", split_axis=0, concat_axis=0, tiled=True),
    )
    program_gross = sum_rows(got_rows, got_labels, program_total)
    program_loss = apply_terms(program_gross, term_table, 3, program_profile)
    return (policy_loss, program_loss)


def solution(mesh):
    placed = (
        P("own", "ev"),
        P("own"),
        P("own"),
        P("own", None),
        P("own"),
        P("own"),
        P("own", None),
        P("own"),
        P("own"),
        P("own"),
        P(),
    )

    def body(ground_up, item_site, item_profile, *rest):
        n = lax.axis_size("own")
        items, cols = ground_up.shape
        sites, pol = rest[2].shape[0], rest[5].shape[0]
        prog = rest[6].shape[0]
        fits = cols % (n * LANES) == 0 and items % LANES == 0 and sites == LANES
        fits = fits and 2 * pol <= LANES and pol % 16 == 0 and prog <= 8
        fits = fits and n % 4 == 0 and n & (n - 1) == 0 and 3 * n <= LANES and 3 * items <= LANES * (LANES - 6)
        return (exchange if fits else shards)(ground_up, item_site, item_profile, *rest)

    return jax.shard_map(
        body,
        mesh=mesh,
        in_specs=placed,
        out_specs=(P("own", "ev"), P("own", "ev")),
        check_vma=False,
    )
```
